32 devices in a mesh: batch: 4 (over y, x), heads: 8 (over z, core).
Axes of the slice: x: 2, y: 2, z: 4, core: 2. Of those that a mesh axis runs over, the one named last changes fastest.
Arguments:
- draft_ids: int32 [192, 8], P('batch'), may hold values from 0 to 50279
- accepted: int32 [192], P('batch'), may hold values from 1 to 8
- embedding: bfloat16 [50280, 2560], P(None, 'heads'), may hold values from -6 to 6
- norm_gain: float32 [2, 2560], replicated, may hold values from 0.5 to 1.5
- w_zx: bfloat16 [2, 2560, 8, 128], P(None, None, 'heads'), may hold values from -0.125 to 0.125
- w_dt: bfloat16 [2, 2560, 8], P(None, None, 'heads'), may hold values from -0.125 to 0.125
- w_bc: bfloat16 [2, 2560, 256], P(None, None, 'heads'), may hold values from -0.125 to 0.125
- dt_bias: float32 [2, 8], P(None, 'heads'), may hold values from -4 to -1
- decay_rate: float32 [2, 8], P(None, 'heads'), may hold values from 1 to 16
- skip_weight: float32 [2, 8], P(None, 'heads'), may hold values from 0.5 to 1.5
- conv_x_w: bfloat16 [2, 4, 512], P(None, None, 'heads'), may hold values from -3 to 3
- conv_x_b: bfloat16 [2, 512], P(None, 'heads'), may hold values from -3 to 3
- conv_bc_w: bfloat16 [2, 4, 256], P(None, None, 'heads'), may hold values from -3 to 3
- conv_bc_b: bfloat16 [2, 256], P(None, 'heads'), may hold values from -3 to 3
- gate_gain: float32 [2, 512], P(None, 'heads'), may hold values from 0.5 to 1.5
- out_w: bfloat16 [2, 512, 2560], P(None, 'heads'), may hold values from -0.375 to 0.375
- ssm_state: float32 [2, 192, 8, 64, 128], P(None, 'batch', 'heads'), may hold values from -1.6 to 1.6
- conv_x_state: bfloat16 [2, 192, 3, 512], P(None, 'batch', None, 'heads'), may hold values from -6 to 6
- conv_bc_state: bfloat16 [2, 192, 3, 256], P(None, 'batch', None, 'heads'), may hold values from -6 to 6
Outputs:
- hidden_out: bfloat16 [1536, 2560], P('batch', 'heads')
- new_ssm: float32 [2, 192, 8, 64, 128], P(None, 'batch', 'heads')
- new_conv_x: bfloat16 [2, 192, 3, 512], P(None, 'batch', None, 'heads')
- new_conv_bc: bfloat16 [2, 192, 3, 256], P(None, 'batch', None, 'heads')
The draws below stay inside these ranges and needn't reach their ends.
Inputs may be any that keep to these rules, and one draw needn't show every extreme that they name: `accepted`: the number of a sequence's draft tokens that are kept, counted from the first.
All inputs are finite; a program needn't handle non-finite values.
Results may differ from the reference program's by a relative error of at most 0.015.
Values may be sent and summed in bfloat16 or wider, within the bound.
A program may use at most 128 MiB of HBM per device.

```python
import math
import jax
import jax.numpy as jnp
import numpy as np
from jax import lax

D = 2560
P_SIZE = 64
N = 128
VOCAB = 50280
KCONV = 4
DRAFT = 8
LAYERS = 2
HEADS = 8
INNER = 512
SEQS = 192


def set_ends(drawn, own_key, least, top_value):
    dims = drawn.shape
    index_at = [jax.random.randint(jax.random.fold_in(own_key, axis), (), 0, dims[axis]) for axis in range(len(dims))]
    drawn = drawn.at[tuple(index_at)].set(least)
    longest = dims.index(max(dims))
    index_at[longest] = (index_at[longest] + 1) % dims[longest]
    return drawn.at[tuple(index_at)].set(top_value)


def strengthened(values, key, source, target, shards_of, factor):
    owner, partner = [(jnp.arange(values.shape[position]) // (values.shape[position] // shards_of)).reshape([-1 if axis == position else 1 for axis in range(values.ndim)]) for position in (source, target)]
    chosen = jax.random.permutation(key, shards_of)[partner]
    strong = (owner == chosen) | (owner == (partner + shards_of // 2) % shards_of)
    return jnp.where(strong, factor * values, values)


def shard_levels(own_key, dims, split, low, largest):
    def one(axis_at, parts):
        heights = jax.random.uniform(jax.random.fold_in(jax.random.fold_in(own_key, 6), axis_at), (parts,), jnp.float32, low / len(split), largest / len(split))
        return jnp.repeat(jnp.exp(heights), dims[axis_at] // parts).reshape((-1,) + (1,) * (len(dims) - axis_at - 1))

    gain = one(*split[0])
    for cut in split[1:]:
        gain = gain * one(*cut)
    return gain


def rank_table(number_of, lean):
    loads = [(1 << 20) // math.isqrt(grade ** lean) + 1 for grade in range(1, number_of + 1)]
    scale = 1 + sum(loads) // (1 << 30)
    return np.cumsum(np.array([max(1, weight // scale) for weight in loads]))


def ranked_ids(stream_key, dims, amount, slope):
    listing = rank_table(amount, slope)
    ticket = jax.random.randint(jax.random.fold_in(stream_key, 1), dims, 0, int(listing[amount - 1]))
    grade = jnp.searchsorted(jnp.asarray(listing, jnp.int32), ticket, side="right")
    return jax.random.permutation(jax.random.fold_in(stream_key, 2), amount)[grade].astype(jnp.int32)


def centred(rng, dims, scale, bound, cuts=(), kind=jnp.bfloat16):
    result = scale * jax.random.normal(rng, dims, jnp.float32)
    if cuts:
        result = result * shard_levels(rng, dims, cuts, -0.22, 0.18)
    return jnp.clip(result, -bound, bound).astype(kind)


def bell_draw_with(key, shape, scale, bound, cuts, heavy, kind=jnp.bfloat16):
    array = scale * jax.random.normal(key, shape, jnp.float32)
    if cuts:
        array = array * shard_levels(key, shape, cuts, -0.22, 0.18)
    return jnp.clip(strengthened(array, jax.random.fold_in(key, 3), *heavy), -bound, bound).astype(kind)


def setup_inputs(seed: int = 0) -> dict:
    seeds = jax.random.split(jax.random.key(seed), 20)
    return {
        "draft_ids": set_ends(ranked_ids(seeds[0], (SEQS, DRAFT), VOCAB, 2), jax.random.fold_in(seeds[0], 3), 0, VOCAB - 1).astype(jnp.int32),
        "accepted": set_ends(jax.random.randint(seeds[1], (SEQS,), 1, DRAFT + 1), jax.random.fold_in(seeds[1], 1), 1, DRAFT).astype(jnp.int32),
        "embedding": centred(seeds[2], (VOCAB, D), 1.0, 6.0, ((1, 8),)),
        "norm_gain": jnp.clip(1.0 + 0.1 * jax.random.normal(seeds[3], (LAYERS, D), jnp.float32), 0.5, 1.5),
        "w_zx": centred(seeds[4], (LAYERS, D, HEADS, 2 * P_SIZE), D ** -0.5, 0.125, ((2, 8),)),
        "w_dt": centred(seeds[5], (LAYERS, D, HEADS), D ** -0.5, 0.125, ((2, 8),)),
        "w_bc": centred(seeds[6], (LAYERS, D, 2 * N), D ** -0.5, 0.125, ((2, 8),)),
        "dt_bias": jnp.clip(-4.0 + 3.0 * jax.random.uniform(seeds[7], (LAYERS, HEADS), jnp.float32) ** shard_levels(seeds[7], (LAYERS, HEADS), ((1, 8),), -0.2, 0.2), -4.0, -1.0),
        "decay_rate": jnp.clip(jnp.exp(math.log(16.0) - 2.7725887 * jax.random.uniform(seeds[8], (LAYERS, HEADS), jnp.float32) ** shard_levels(seeds[8], (LAYERS, HEADS), ((1, 8),), -0.2, 0.2)), 1.0, 16.0),
        "skip_weight": jnp.clip(0.5 + 1.0 * jax.random.uniform(seeds[9], (LAYERS, HEADS), jnp.float32) ** shard_levels(seeds[9], (LAYERS, HEADS), ((1, 8),), -0.2, 0.2), 0.5, 1.5),
        "conv_x_w": centred(seeds[10], (LAYERS, KCONV, INNER), 0.5, 3.0, ((2, 8),)),
        "conv_x_b": centred(seeds[11], (LAYERS, INNER), 0.5, 3.0, ((1, 8),)),
        "conv_bc_w": centred(seeds[12], (LAYERS, KCONV, 2 * N), 0.5, 3.0, ((2, 8),)),
        "conv_bc_b": centred(seeds[13], (LAYERS, 2 * N), 0.5, 3.0, ((1, 8),)),
        "gate_gain": jnp.clip(1.0 + 0.1 * jax.random.normal(seeds[14], (LAYERS, INNER), jnp.float32), 0.5, 1.5),
        "out_w": bell_draw_with(seeds[15], (LAYERS, INNER, D), INNER ** -0.5, 0.375, ((1, 8),), (1, 2, 8, 2.0)),
        "ssm_state": centred(seeds[16], (LAYERS, SEQS, HEADS, P_SIZE, N), 0.2, 1.6, ((1, 4), (2, 8)), jnp.float32),
        "conv_x_state": centred(seeds[17], (LAYERS, SEQS, KCONV - 1, INNER), 1.0, 6.0, ((1, 4), (3, 8))),
        "conv_bc_state": centred(seeds[18], (LAYERS, SEQS, KCONV - 1, 2 * N), 1.0, 6.0, ((1, 4), (3, 8))),
    }


EPS = 1e-05

def rms_scale(total, count):
    return lax.rsqrt(total / count + EPS)

def convolve(window, weight, bias, count):
    weight = weight.astype(jnp.float32)
    acc = window[:, 0:count] * weight[0]
    for k in range(1, weight.shape[0]):
        acc = acc + window[:, k:k + count] * weight[k]
    return jax.nn.silu(acc + bias.astype(jnp.float32))

def keep_rows(window, accepted, kept_rows):
    last_start = window.shape[1] - kept_rows
    kept = window[:, 1:1 + kept_rows]
    for start in range(2, last_start + 1):
        kept = jnp.where((accepted == start)[:, None, None], window[:, start:start + kept_rows], kept)
    return kept

def recur(decay, step, values, bmat, cmat, skip, state, accepted):
    kept = state
    outputs = []
    for t in range(values.shape[1]):
        state = decay[:, t, None, None] * state + (step[:, t, None] * values[:, t])[:, :, None] * bmat[:, t, None, :]
        outputs.append(lax.optimization_barrier(jnp.sum(state * cmat[:, t, None, :], axis=-1)) + skip * values[:, t])
        kept = jnp.where((accepted == t + 1)[:, None, None], state, kept)
    return (jnp.stack(outputs, 1), kept)

def reference(draft_ids, accepted, embedding, norm_gain, w_zx, w_dt, w_bc, dt_bias, decay_rate, skip_weight, conv_x_w, conv_x_b, conv_bc_w, conv_bc_b, gate_gain, out_w, ssm_state, conv_x_state, conv_bc_state):
    seqs, draft = draft_ids.shape
    heads = w_zx.shape[2]
    width = w_zx.shape[3] // 2
    inner = heads * width
    model = embedding.shape[1]
    states = w_bc.shape[2] // 2
    kernel = conv_x_w.shape[1]
    stream = embedding[draft_ids.reshape(-1)]
    saved_state, saved_x, saved_bc = ([], [], [])
    for layer in range(LAYERS):
        value = stream.astype(jnp.float32)
        normed = (value * rms_scale(lax.optimization_barrier(jnp.sum(value * value, -1, keepdims=True)), model) * norm_gain[layer]).astype(jnp.bfloat16)
        zx = jnp.dot(normed, w_zx[layer].reshape(model, -1), preferred_element_type=jnp.float32).astype(jnp.bfloat16)
        zx = zx.reshape(seqs, draft, heads, 2, width)
        gate_z = zx[:, :, :, 0].astype(jnp.float32)
        values = zx[:, :, :, 1].reshape(seqs, draft, inner)
        dt_raw = jnp.dot(normed, w_dt[layer], preferred_element_type=jnp.float32).astype(jnp.bfloat16).reshape(seqs, draft, heads)
        bc = jnp.dot(normed, w_bc[layer], preferred_element_type=jnp.float32).astype(jnp.bfloat16).reshape(seqs, draft, 2 * states)
        window_x = jnp.concatenate([conv_x_state[layer], values], axis=1)
        xc = convolve(window_x.astype(jnp.float32), conv_x_w[layer], conv_x_b[layer], draft).reshape(seqs, draft, heads, width)
        window_bc = jnp.concatenate([conv_bc_state[layer], bc], axis=1)
        bcc = convolve(window_bc.astype(jnp.float32), conv_bc_w[layer], conv_bc_b[layer], draft).astype(jnp.bfloat16)
        bcc = lax.optimization_barrier(bcc).astype(jnp.float32)
        bmat = bcc[..., :states]
        cmat = bcc[..., states:]
        step = jax.nn.softplus(dt_raw.astype(jnp.float32) + dt_bias[layer])
        decay = jnp.exp(-step * decay_rate[layer])

        def run(pieces):
            return recur(pieces[0], pieces[1], pieces[2], bmat, cmat, pieces[3], pieces[4], accepted)
        outputs, kept = lax.map(run, (jnp.moveaxis(decay, 2, 0), jnp.moveaxis(step, 2, 0), jnp.moveaxis(xc, 2, 0), skip_weight[layer], jnp.moveaxis(ssm_state[layer], 1, 0)))
        outputs = jnp.moveaxis(outputs, 0, 2)
        saved_state.append(jnp.moveaxis(kept, 0, 1))
        saved_x.append(keep_rows(window_x, accepted, kernel - 1))
        saved_bc.append(keep_rows(window_bc, accepted, kernel - 1))
        gated = outputs * jax.nn.silu(gate_z)
        ssq = lax.optimization_barrier(jnp.sum(gated * gated, axis=(2, 3))).reshape(-1)
        u = (gated.reshape(seqs, draft, inner) * gate_gain[layer]).astype(jnp.bfloat16).reshape(-1, inner)
        mix = jnp.dot(u, out_w[layer], preferred_element_type=jnp.float32) * rms_scale(ssq, inner)[:, None]
        stream = (stream.astype(jnp.float32) + mix).astype(jnp.bfloat16)
    return (stream, jnp.stack(saved_state), jnp.stack(saved_x), jnp.stack(saved_bc))
```

```python
import functools

import jax
import jax.numpy as jnp
from jax import lax
from jax.experimental import pallas as pl
from jax.experimental.pallas import tpu as pltpu
from jax.sharding import PartitionSpec as P

LAYERS = 2
EPS = 1e-05
MESH = pl.DeviceIdType.MESH
CHUNK = 2048
VMEM_LIMIT = 60 * 1024 * 1024


def rms_scale(total, count):
    return lax.rsqrt(total / count + EPS)


def dot_tn(a, b):
    return lax.dot_general(a, b, (((0,), (0,)), ((), ())), preferred_element_type=jnp.float32)


def dot_nt(a, b):
    return lax.dot_general(a, b, (((1,), (1,)), ((), ())), preferred_element_type=jnp.float32)


def keep_rows(window, accepted, kept_rows):
    last_start = window.shape[1] - kept_rows
    kept = window[:, 1 : 1 + kept_rows]
    for start in range(2, last_start + 1):
        kept = jnp.where(
            (accepted == start)[:, None, None], window[:, start : start + kept_rows], kept
        )
    return kept


def greet(n):
    me = lax.axis_index("heads")
    barrier = pltpu.get_barrier_semaphore()
    for d in range(1, n):
        pl.semaphore_signal(
            barrier, inc=1, device_id={"heads": lax.rem(me + d, n)}, device_id_type=MESH
        )
    pl.semaphore_wait(barrier, n - 1)


class Gather:
    def __init__(self, n, src, out, send, recv, fsend, frecv):
        self.n, self.src, self.out = n, src, out
        self.send, self.recv, self.fsend, self.frecv = send, recv, fsend, frecv
        self.me = lax.axis_index("heads")
        self.core = lax.rem(self.me, 2)
        self.chip = self.me // 2
        self.chips = n // 2
        self.mate = self.me + 1 - 2 * self.core

    def slot(self, c, core):
        return 2 * lax.rem(self.chip + self.chips - c, self.chips) + core

    def copy(self, src, slot, device, send, recv):
        return pltpu.make_async_remote_copy(
            src_ref=src,
            dst_ref=self.out.at[slot],
            send_sem=send,
            recv_sem=recv,
            device_id={"heads": device},
            device_id_type=MESH,
        )

    def first(self, c):
        if c == 0:
            return self.copy(self.src, self.me, self.mate, self.send.at[0], self.recv.at[0])
        dst = 2 * lax.rem(self.chip + c, self.chips) + self.core
        return self.copy(self.src, self.me, dst, self.send.at[c], self.recv.at[c])

    def arrival(self, c):
        if c == 0:
            return self.copy(self.src, self.mate, self.mate, self.send.at[0], self.recv.at[0])
        slot = self.slot(c, self.core)
        return self.copy(self.src, slot, slot, self.send.at[c], self.recv.at[c])

    def forward(self, c):
        slot = self.slot(c, self.core)
        return self.copy(
            self.out.at[slot], slot, self.mate, self.fsend.at[c], self.frecv.at[c]
        )

    def forwarded(self, c):
        slot = self.slot(c, 1 - self.core)
        return self.copy(
            self.out.at[slot], slot, self.mate, self.fsend.at[c], self.frecv.at[c]
        )

    def order(self):
        return sorted(range(1, self.chips), key=lambda c: min(c, self.chips - c))

    def start(self):
        for c in self.order():
            self.first(c).start()
        self.first(0).start()

    def relay(self):
        for c in self.order():
            self.arrival(c).wait_recv()
            self.forward(c).start()

    def finish(self):
        for c in range(self.chips):
            self.first(c).wait_send()
        self.arrival(0).wait_recv()
        for c in range(1, self.chips):
            self.forwarded(c).wait_recv()
            self.forward(c).wait_send()


def gather_sems(n, count):
    return [pltpu.SemaphoreType.DMA((n // 2,))] * (4 * count)


def ag_kernel(n, count, *refs):
    srcs, outs = refs[:count], refs[count : 2 * count]
    sems, local = refs[2 * count : -1], refs[-1]
    greet(n)
    me = lax.axis_index("heads")
    gathers = [
        Gather(n, srcs[i], outs[i], *sems[4 * i : 4 * i + 4]) for i in range(count)
    ]
    owns = [
        pltpu.make_async_copy(srcs[i], outs[i].at[me], local.at[i]) for i in range(count)
    ]
    for g in gathers:
        g.start()
    for own in owns:
        own.start()
    for g in gathers:
        g.relay()
    for g in gathers:
        g.finish()
    for own in owns:
        own.wait()


def all_gather(arrays, n, cid):
    count = len(arrays)
    return pl.pallas_call(
        functools.partial(ag_kernel, n, count),
        out_shape=[jax.ShapeDtypeStruct((n,) + a.shape, a.dtype) for a in arrays],
        in_specs=[pl.BlockSpec(memory_space=pltpu.VMEM)] * count,
        out_specs=[pl.BlockSpec(memory_space=pltpu.VMEM)] * count,
        scratch_shapes=gather_sems(n, count) + [pltpu.SemaphoreType.DMA((count,))],
        compiler_params=pltpu.CompilerParams(
            collective_id=cid, has_side_effects=True, vmem_limit_bytes=VMEM_LIMIT
        ),
        name=f"gather_{cid}",
    )(*arrays)


def lookup_kernel(
    n, vocab, ids, table, whole, parts, part_out, whole_out, parts_out, acc,
    s0, s1, s2, s3, psend, precv, local
):
    step = pl.program_id(0)
    steps = pl.num_programs(0)
    me = lax.axis_index("heads")
    gather = Gather(n, whole, whole_out, s0, s1, s2, s3)

    def exchange(d):
        dst = lax.rem(me + d, n)
        return pltpu.make_async_remote_copy(
            src_ref=parts.at[dst],
            dst_ref=parts_out.at[me],
            send_sem=psend.at[d],
            recv_sem=precv.at[d],
            device_id={"heads": dst},
            device_id_type=MESH,
        )

    def came(d):
        src = lax.rem(me + n - d, n)
        return pltpu.make_async_remote_copy(
            src_ref=parts.at[src],
            dst_ref=parts_out.at[src],
            send_sem=psend.at[d],
            recv_sem=precv.at[d],
            device_id={"heads": src},
            device_id_type=MESH,
        )

    own_whole = pltpu.make_async_copy(whole, whole_out.at[me], local.at[0])
    own_part = pltpu.make_async_copy(parts.at[me], parts_out.at[me], local.at[1])

    @pl.when(step == 0)
    def _():
        greet(n)
        gather.start()
        for d in range(1, n):
            exchange(d).start()
        own_whole.start()
        own_part.start()
        acc[...] = jnp.zeros_like(acc)

    base = step * CHUNK
    rows = lax.broadcasted_iota(jnp.int32, (CHUNK, ids.shape[1]), 0) + base
    hot = jnp.where(rows == ids[...], 1.0, 0.0).astype(jnp.bfloat16)

    @pl.when(step < steps - 1)
    def _():
        acc[...] += jnp.dot(table[...], hot, preferred_element_type=jnp.float32)

    @pl.when(step == steps - 1)
    def _():
        columns = lax.broadcasted_iota(jnp.int32, table.shape, 1) + base
        block = jnp.where(columns < vocab, table[...].astype(jnp.float32), 0.0)
        total = acc[...] + jnp.dot(
            block.astype(jnp.bfloat16), hot, preferred_element_type=jnp.float32
        )
        part_out[...] = total.astype(jnp.bfloat16)
        gather.relay()
        gather.finish()
        for d in range(1, n):
            exchange(d).wait_send()
            came(d).wait_recv()
        own_whole.wait()
        own_part.wait()


def lookup(ids, table, whole, parts, n):
    cols, vocab = table.shape
    tokens = ids.shape[1]
    anywhere = pl.BlockSpec(memory_space=pl.ANY)
    return pl.pallas_call(
        functools.partial(lookup_kernel, n, vocab),
        grid=(pl.cdiv(vocab, CHUNK),),
        out_shape=[
            jax.ShapeDtypeStruct((cols, tokens), jnp.bfloat16),
            jax.ShapeDtypeStruct((n,) + whole.shape, whole.dtype),
            jax.ShapeDtypeStruct(parts.shape, parts.dtype),
        ],
        in_specs=[
            pl.BlockSpec((1, tokens), lambda i: (0, 0)),
            pl.BlockSpec((cols, CHUNK), lambda i: (0, i)),
            anywhere,
            anywhere,
        ],
        out_specs=[pl.BlockSpec((cols, tokens), lambda i: (0, 0)), anywhere, anywhere],
        scratch_shapes=[pltpu.VMEM((cols, tokens), jnp.float32)]
        + gather_sems(n, 1)
        + [
            pltpu.SemaphoreType.DMA((n,)),
            pltpu.SemaphoreType.DMA((n,)),
            pltpu.SemaphoreType.DMA((2,)),
        ],
        compiler_params=pltpu.CompilerParams(
            collective_id=0,
            has_side_effects=True,
            vmem_limit_bytes=VMEM_LIMIT,
            dimension_semantics=("arbitrary",),
        ),
        name="lookup",
    )(ids, table, whole, parts)


def conv_rows(x, state, taps, draft):
    tokens, channels = x.shape
    x3 = x.reshape(tokens // draft, draft, channels)
    s3 = state.reshape(tokens // draft, draft, channels)
    at = lax.broadcasted_iota(jnp.int32, (1, draft, channels), 1)
    kernel = taps.shape[0] - 1
    acc = None
    for k in range(kernel):
        back = kernel - 1 - k
        seen = x3
        if back:
            seen = jnp.where(at >= back, pltpu.roll(x3, back, 1), pltpu.roll(s3, back, 1))
        term = seen * taps[k : k + 1, :][None]
        acc = term if acc is None else acc + term
    acc = (acc + taps[kernel : kernel + 1, :][None]).reshape(tokens, channels)
    return acc * (1.0 / (1.0 + jnp.exp(-acc)))


def mixer_kernel(
    draft, zx, dt, bc_t, bc_state_t, bc_taps, x_state, x_taps, heads3, accepted, gain, h0,
    u_t, ssq, h_new, c_ref, y_ref, keep_ref
):
    tokens = zx.shape[0]
    width = zx.shape[1] // 2
    states = bc_t.shape[0] // 2
    f32, bf16 = jnp.float32, jnp.bfloat16
    bc = jnp.transpose(bc_t[...].astype(f32))
    bc_state = jnp.transpose(bc_state_t[...].astype(f32))
    bcc = conv_rows(bc, bc_state, bc_taps[...], draft)
    b = bcc[:, :states].astype(bf16)
    c = bcc[:, states:].astype(bf16)
    c_ref[...] = c.astype(f32)
    zx_all = zx[...].astype(f32)
    xc = conv_rows(zx_all[:, width:], x_state[...].astype(f32), x_taps[...], draft)
    bias, rate, skip = heads3[0:1, 0:1], heads3[1:2, 0:1], heads3[2:3, 0:1]
    raw = dt[...] + bias
    step_row = jnp.maximum(raw, 0.0) + jnp.log1p(jnp.exp(-jnp.abs(raw)))
    row = lax.broadcasted_iota(jnp.int32, (tokens, tokens), 0)
    col = lax.broadcasted_iota(jnp.int32, (tokens, tokens), 1)
    same = (row // draft == col // draft) & (col <= row)
    eye = row == col
    steps_col = jnp.sum(jnp.where(eye, step_row, 0.0), axis=1, keepdims=True)
    sum_col = jnp.sum(jnp.where(same, step_row, 0.0), axis=1, keepdims=True)
    sum_row = jnp.sum(jnp.where(eye, sum_col, 0.0), axis=0, keepdims=True)
    spread = jnp.exp(jnp.where(same, (sum_row - sum_col) * rate, -1e30))
    scores = dot_nt(c, b) * spread
    xw = xc * steps_col
    y = jnp.dot(scores.astype(bf16), xw.astype(bf16), preferred_element_type=f32)

    at = lax.broadcasted_iota(jnp.int32, (tokens, 1), 0) % draft
    kept = accepted[...]
    seqs = tokens // draft
    last = jnp.where(at == kept - 1, sum_col, 0.0).reshape(seqs, draft, 1)
    last = jnp.broadcast_to(jnp.sum(last, axis=1, keepdims=True), (seqs, draft, 1))
    last = last.reshape(tokens, 1)
    coef = jnp.exp(jnp.where(at < kept, (sum_col - last) * rate, -1e30))
    keep_ref[...] = jnp.broadcast_to(jnp.exp(-last * rate), keep_ref.shape)
    xk_t = jnp.transpose(xw * coef).astype(bf16)
    lanes = 128
    in_group = lanes // draft
    group_row = lax.broadcasted_iota(jnp.int32, (lanes, states), 0) // draft
    for q in range(seqs):
        rows = slice(q * draft, (q + 1) * draft)
        g = q // in_group
        state = h0[q]
        y_ref[rows, :] = dot_nt(c_ref[rows, :].astype(bf16), state.astype(bf16))
        mine = jnp.where(
            group_row == q % in_group, b[g * lanes : (g + 1) * lanes].astype(f32), 0.0
        )
        added = jnp.dot(
            xk_t[:, g * lanes : (g + 1) * lanes],
            mine.astype(bf16),
            preferred_element_type=f32,
        )
        h_new[q] = keep_ref[q * draft : q * draft + 1, :] * state + added
    y = y + jnp.exp(-sum_col * rate) * y_ref[...] + skip * xc
    z = zx_all[:, :width]
    gated = y * (z * (1.0 / (1.0 + jnp.exp(-z))))
    u = gated * gain[...]
    u_t[...] = jnp.transpose(u).astype(bf16)
    gated_t = jnp.transpose(gated)
    ssq[...] = jnp.broadcast_to(jnp.sum(gated_t * gated_t, axis=0, keepdims=True), ssq.shape)


def mix_tokens(draft, zx, h0, *rest):
    tokens, width = zx.shape[0], zx.shape[1] // 2
    states = h0.shape[2]
    count = 2 + len(rest)
    return pl.pallas_call(
        functools.partial(mixer_kernel, draft),
        out_shape=[
            jax.ShapeDtypeStruct((width, tokens), jnp.bfloat16),
            jax.ShapeDtypeStruct((8, tokens), jnp.float32),
            jax.ShapeDtypeStruct(h0.shape, jnp.float32),
        ],
        in_specs=[pl.BlockSpec(memory_space=pltpu.VMEM)] * count,
        out_specs=[pl.BlockSpec(memory_space=pltpu.VMEM)] * 3,
        scratch_shapes=[
            pltpu.VMEM((tokens, states), jnp.float32),
            pltpu.VMEM((tokens, width), jnp.float32),
            pltpu.VMEM((tokens, states), jnp.float32),
        ],
        compiler_params=pltpu.CompilerParams(vmem_limit_bytes=VMEM_LIMIT),
        name="mixer",
    )(zx, *rest, h0)


def local(
    draft_ids, accepted, embedding, norm_gain, w_zx, w_dt, w_bc, dt_bias, decay_rate,
    skip_weight, conv_x_w, conv_x_b, conv_bc_w, conv_bc_b, gate_gain, out_w, ssm_state,
    conv_x_state, conv_bc_state,
):
    f32, bf16 = jnp.float32, jnp.bfloat16
    n = lax.axis_size("heads")
    seqs, draft = draft_ids.shape
    tokens = seqs * draft
    width = w_zx.shape[3] // 2
    own_cols = embedding.shape[1]
    model = own_cols * n
    inner = width * n
    bc_here = w_bc.shape[2]
    kernel = conv_x_w.shape[1]
    me = lax.axis_index("heads")

    rows_before = draft - (kernel - 1)
    bc_pad = jnp.pad(conv_bc_state, ((0, 0), (0, 0), (rows_before, 0), (0, 0)))
    bc_pad = bc_pad.transpose(0, 3, 1, 2).reshape(LAYERS, bc_here, tokens)
    x_pad = jnp.pad(conv_x_state, ((0, 0), (0, 0), (rows_before, 0), (0, 0)))
    x_pad = x_pad.reshape(LAYERS, tokens, width)
    bc_taps = jnp.concatenate([conv_bc_w, conv_bc_b[:, None]], axis=1).transpose(0, 2, 1)
    bc_taps = jnp.pad(bc_taps, ((0, 0), (0, 0), (0, 128 - kernel - 1)))
    x_taps = jnp.concatenate([conv_x_w, conv_x_b[:, None]], axis=1).astype(f32)
    heads3 = jnp.stack([dt_bias, decay_rate, skip_weight], axis=1)
    kept = jnp.repeat(accepted, draft)[:, None]
    w_bd = jnp.concatenate([w_bc.transpose(0, 2, 1), w_dt.transpose(0, 2, 1)], axis=1)

    parts = out_w[1].reshape(width, n, own_cols).transpose(1, 0, 2)
    part, out_whole, out_mine = lookup(
        draft_ids.reshape(1, tokens), embedding.T, out_w[0], parts, n
    )
    stream, bc_pad_all, bc_taps_all = all_gather([part, bc_pad, bc_taps], n, 1)
    stream = stream.reshape(model, tokens)
    bc_pad_all = bc_pad_all.transpose(1, 0, 2, 3).reshape(LAYERS, n * bc_here, tokens)
    bc_taps_all = bc_taps_all[..., : kernel + 1].transpose(1, 3, 0, 2)
    bc_taps_all = bc_taps_all.reshape(LAYERS, kernel + 1, n * bc_here).astype(f32)
    saved_state, saved_x, saved_bc = [], [], []
    result = None
    for layer in range(LAYERS):
        value = stream.astype(f32)
        normed = (
            value
            * rms_scale(jnp.sum(value * value, 0, keepdims=True), model)
            * norm_gain[layer][:, None]
        ).astype(bf16)
        zx = dot_tn(normed, w_zx[layer].reshape(model, -1)).astype(bf16)
        bd = jnp.dot(w_bd[layer], normed, preferred_element_type=f32).astype(bf16)
        bc_t = bd[:bc_here]
        dt = bd[bc_here:].astype(f32)
        (bc_all,) = all_gather([bc_t], n, 2 + 2 * layer)
        u_t, ssq, h_new = mix_tokens(
            draft, zx, ssm_state[layer].reshape(seqs, width, -1), dt,
            bc_all.reshape(n * bc_here, tokens), bc_pad_all[layer], bc_taps_all[layer],
            x_pad[layer], x_taps[layer], heads3[layer], kept, gate_gain[layer][None],
        )
        saved_state.append(h_new.reshape(ssm_state.shape[1:]))
        window_x = jnp.concatenate(
            [conv_x_state[layer], zx[:, width:].reshape(seqs, draft, width)], axis=1
        )
        saved_x.append(keep_rows(window_x, accepted, kernel - 1))
        window_bc = jnp.concatenate(
            [conv_bc_state[layer], bc_t.T.reshape(seqs, draft, bc_here)], axis=1
        )
        saved_bc.append(keep_rows(window_bc, accepted, kernel - 1))
        u_all, ssq_all = all_gather([u_t, ssq], n, 3 + 2 * layer)
        u_all = u_all.reshape(inner, tokens)
        scale = rms_scale(jnp.sum(ssq_all[:, 0], axis=0), inner)[None]
        if layer + 1 < LAYERS:
            mix = dot_tn(out_whole.reshape(inner, model), u_all) * scale
            stream = (value + mix).astype(bf16)
        else:
            mix = dot_tn(out_mine.reshape(inner, own_cols), u_all) * scale
            mine = lax.dynamic_slice_in_dim(stream, me * own_cols, own_cols, 0)
            result = (mine.astype(f32) + mix).astype(bf16).T
    return (result, jnp.stack(saved_state), jnp.stack(saved_x), jnp.stack(saved_bc))


def solution(mesh):
    placed = (
        P("batch", None),
        P("batch"),
        P(None, "heads"),
        P(),
        P(None, None, "heads", None),
        P(None, None, "heads"),
        P(None, None, "heads"),
        P(None, "heads"),
        P(None, "heads"),
        P(None, "heads"),
        P(None, None, "heads"),
        P(None, "heads"),
        P(None, None, "heads"),
        P(None, "heads"),
        P(None, "heads"),
        P(None, "heads", None),
        P(None, "batch", "heads", None, None),
        P(None, "batch", None, "heads"),
        P(None, "batch", None, "heads"),
    )
    return jax.shard_map(
        local,
        mesh=mesh,
        in_specs=placed,
        out_specs=(
            P("batch", "heads"),
            P(None, "batch", "heads", None, None),
            P(None, "batch", None, "heads"),
            P(None, "batch", None, "heads"),
        ),
        check_vma=False,
    )
```

```python
import functools

import jax
import jax.numpy as jnp
from jax import lax
from jax.experimental import pallas as pl
from jax.experimental.pallas import tpu as pltpu
from jax.sharding import PartitionSpec as P

LAYERS = 2
EPS = 1e-05
MESH = pl.DeviceIdType.MESH
CHUNK = 2048
VMEM_LIMIT = 60 * 1024 * 1024


def rms_scale(total, count):
    return lax.rsqrt(total / count + EPS)


def dot_tn(a, b):
    return lax.dot_general(a, b, (((0,), (0,)), ((), ())), preferred_element_type=jnp.float32)


def dot_nt(a, b):
    return lax.dot_general(a, b, (((1,), (1,)), ((), ())), preferred_element_type=jnp.float32)


def keep_rows(window, accepted, kept_rows):
    last_start = window.shape[1] - kept_rows
    kept = window[:, 1 : 1 + kept_rows]
    for start in range(2, last_start + 1):
        kept = jnp.where(
            (accepted == start)[:, None, None], window[:, start : start + kept_rows], kept
        )
    return kept


def greet(n):
    me = lax.axis_index("heads")
    barrier = pltpu.get_barrier_semaphore()
    for d in range(1, n):
        pl.semaphore_signal(
            barrier, inc=1, device_id={"heads": lax.rem(me + d, n)}, device_id_type=MESH
        )
    pl.semaphore_wait(barrier, n - 1)


class Gather:
    def __init__(self, n, src, out, send, recv, fsend, frecv):
        self.n, self.src, self.out = n, src, out
        self.send, self.recv, self.fsend, self.frecv = send, recv, fsend, frecv
        self.me = lax.axis_index("heads")
        self.core = lax.rem(self.me, 2)
        self.chip = self.me // 2
        self.chips = n // 2
        self.mate = self.me + 1 - 2 * self.core

    def copy(self, src, slot, device, send, recv):
        return pltpu.make_async_remote_copy(
            src_ref=src,
            dst_ref=self.out.at[slot],
            send_sem=send,
            recv_sem=recv,
            device_id={"heads": device},
            device_id_type=MESH,
        )

    def index(self, side, c):
        return c if side < 0 else self.chips - 1 + c

    def has(self, side, c):
        return self.chip >= c if side < 0 else self.chip + c < self.chips

    def slot(self, side, c, core):
        return 2 * (self.chip + side * c) + core

    def hop(self, side, c):
        i = self.index(side, c + 1)
        slot = self.me if c == 0 else self.slot(side, c, self.core)
        src = self.src if c == 0 else self.out.at[slot]
        return self.copy(src, slot, self.slot(-side, 1, self.core), self.send.at[i], self.recv.at[i])

    def arrival(self, side, c):
        i = self.index(side, c)
        slot = self.slot(side, c, self.core)
        return self.copy(
            self.src, slot, self.slot(side, 1, self.core), self.send.at[i], self.recv.at[i]
        )

    def across(self, side, c, core):
        i = self.index(side, c)
        slot = self.slot(side, c, core)
        return self.copy(self.out.at[slot], slot, self.mate, self.fsend.at[i], self.frecv.at[i])

    def first(self, slot):
        return self.copy(self.src, slot, self.mate, self.send.at[0], self.recv.at[0])

    def places(self):
        return [(side, c) for c in range(1, self.chips) for side in (-1, 1)]

    def start(self):
        for side in (-1, 1):
            pl.when(self.has(-side, 1))(lambda side=side: self.hop(side, 0).start())
        self.first(self.me).start()

    def relay(self):
        for side, c in self.places():

            @pl.when(self.has(side, c))
            def _():
                self.arrival(side, c).wait_recv()

            @pl.when(self.has(side, c) & self.has(-side, 1))
            def _():
                self.hop(side, c).start()

            @pl.when(self.has(side, c))
            def _():
                self.across(side, c, self.core).start()

    def finish(self):
        self.first(self.me).wait_send()
        self.first(self.mate).wait_recv()
        for side in (-1, 1):
            pl.when(self.has(-side, 1))(lambda side=side: self.hop(side, 0).wait_send())
        for side, c in self.places():

            @pl.when(self.has(side, c) & self.has(-side, 1))
            def _():
                self.hop(side, c).wait_send()

            @pl.when(self.has(side, c))
            def _():
                self.across(side, c, 1 - self.core).wait_recv()
                self.across(side, c, self.core).wait_send()


def gather_sems(n, count):
    return [pltpu.SemaphoreType.DMA((n,))] * (4 * count)


def ag_kernel(n, count, *refs):
    srcs, outs = refs[:count], refs[count : 2 * count]
    sems, local = refs[2 * count : -1], refs[-1]
    greet(n)
    me = lax.axis_index("heads")
    gathers = [
        Gather(n, srcs[i], outs[i], *sems[4 * i : 4 * i + 4]) for i in range(count)
    ]
    owns = [
        pltpu.make_async_copy(srcs[i], outs[i].at[me], local.at[i]) for i in range(count)
    ]
    for g in gathers:
        g.start()
    for own in owns:
        own.start()
    for g in gathers:
        g.relay()
    for g in gathers:
        g.finish()
    for own in owns:
        own.wait()


def all_gather(arrays, n, cid):
    count = len(arrays)
    return pl.pallas_call(
        functools.partial(ag_kernel, n, count),
        out_shape=[jax.ShapeDtypeStruct((n,) + a.shape, a.dtype) for a in arrays],
        in_specs=[pl.BlockSpec(memory_space=pltpu.VMEM)] * count,
        out_specs=[pl.BlockSpec(memory_space=pltpu.VMEM)] * count,
        scratch_shapes=gather_sems(n, count) + [pltpu.SemaphoreType.DMA((count,))],
        compiler_params=pltpu.CompilerParams(
            collective_id=cid, has_side_effects=True, vmem_limit_bytes=VMEM_LIMIT
        ),
        name=f"gather_{cid}",
    )(*arrays)


def lookup_kernel(
    n, vocab, ids, table, whole, parts, part_out, whole_out, parts_out, acc,
    s0, s1, s2, s3, psend, precv, local
):
    step = pl.program_id(0)
    steps = pl.num_programs(0)
    me = lax.axis_index("heads")
    gather = Gather(n, whole, whole_out, s0, s1, s2, s3)

    def exchange(d):
        dst = lax.rem(me + d, n)
        return pltpu.make_async_remote_copy(
            src_ref=parts.at[dst],
            dst_ref=parts_out.at[me],
            send_sem=psend.at[d],
            recv_sem=precv.at[d],
            device_id={"heads": dst},
            device_id_type=MESH,
        )

    def came(d):
        src = lax.rem(me + n - d, n)
        return pltpu.make_async_remote_copy(
            src_ref=parts.at[src],
            dst_ref=parts_out.at[src],
            send_sem=psend.at[d],
            recv_sem=precv.at[d],
            device_id={"heads": src},
            device_id_type=MESH,
        )

    own_whole = pltpu.make_async_copy(whole, whole_out.at[me], local.at[0])
    own_part = pltpu.make_async_copy(parts.at[me], parts_out.at[me], local.at[1])

    @pl.when(step == 0)
    def _():
        greet(n)
        gather.start()
        for d in range(1, n):
            exchange(d).start()
        own_whole.start()
        own_part.start()
        acc[...] = jnp.zeros_like(acc)

    base = step * CHUNK
    rows = lax.broadcasted_iota(jnp.int32, (CHUNK, ids.shape[1]), 0) + base
    hot = jnp.where(rows == ids[...], 1.0, 0.0).astype(jnp.bfloat16)

    @pl.when(step < steps - 1)
    def _():
        acc[...] += jnp.dot(table[...], hot, preferred_element_type=jnp.float32)

    @pl.when(step == steps - 1)
    def _():
        columns = lax.broadcasted_iota(jnp.int32, table.shape, 1) + base
        block = jnp.where(columns < vocab, table[...].astype(jnp.float32), 0.0)
        total = acc[...] + jnp.dot(
            block.astype(jnp.bfloat16), hot, preferred_element_type=jnp.float32
        )
        part_out[...] = total.astype(jnp.bfloat16)
        gather.relay()
        gather.finish()
        for d in range(1, n):
            exchange(d).wait_send()
            came(d).wait_recv()
        own_whole.wait()
        own_part.wait()


def lookup(ids, table, whole, parts, n):
    cols, vocab = table.shape
    tokens = ids.shape[1]
    anywhere = pl.BlockSpec(memory_space=pl.ANY)
    return pl.pallas_call(
        functools.partial(lookup_kernel, n, vocab),
        grid=(pl.cdiv(vocab, CHUNK),),
        out_shape=[
            jax.ShapeDtypeStruct((cols, tokens), jnp.bfloat16),
            jax.ShapeDtypeStruct((n,) + whole.shape, whole.dtype),
            jax.ShapeDtypeStruct(parts.shape, parts.dtype),
        ],
        in_specs=[
            pl.BlockSpec((1, tokens), lambda i: (0, 0)),
            pl.BlockSpec((cols, CHUNK), lambda i: (0, i)),
            anywhere,
            anywhere,
        ],
        out_specs=[pl.BlockSpec((cols, tokens), lambda i: (0, 0)), anywhere, anywhere],
        scratch_shapes=[pltpu.VMEM((cols, tokens), jnp.float32)]
        + gather_sems(n, 1)
        + [
            pltpu.SemaphoreType.DMA((n,)),
            pltpu.SemaphoreType.DMA((n,)),
            pltpu.SemaphoreType.DMA((2,)),
        ],
        compiler_params=pltpu.CompilerParams(
            collective_id=0,
            has_side_effects=True,
            vmem_limit_bytes=VMEM_LIMIT,
            dimension_semantics=("arbitrary",),
        ),
        name="lookup",
    )(ids, table, whole, parts)


def conv_rows(x, state, taps, draft):
    tokens, channels = x.shape
    x3 = x.reshape(tokens // draft, draft, channels)
    s3 = state.reshape(tokens // draft, draft, channels)
    at = lax.broadcasted_iota(jnp.int32, (1, draft, channels), 1)
    kernel = taps.shape[0] - 1
    acc = None
    for k in range(kernel):
        back = kernel - 1 - k
        seen = x3
        if back:
            seen = jnp.where(at >= back, pltpu.roll(x3, back, 1), pltpu.roll(s3, back, 1))
        term = seen * taps[k : k + 1, :][None]
        acc = term if acc is None else acc + term
    acc = (acc + taps[kernel : kernel + 1, :][None]).reshape(tokens, channels)
    return acc * (1.0 / (1.0 + jnp.exp(-acc)))


def mixer_kernel(
    draft, zx, dt, bc_t, bc_state_t, bc_taps, x_state, x_taps, heads3, accepted, gain, h0,
    u_t, ssq, h_new, c_ref, y_ref, keep_ref
):
    tokens = zx.shape[0]
    width = zx.shape[1] // 2
    states = bc_t.shape[0] // 2
    f32, bf16 = jnp.float32, jnp.bfloat16
    bc = jnp.transpose(bc_t[...].astype(f32))
    bc_state = jnp.transpose(bc_state_t[...].astype(f32))
    bcc = conv_rows(bc, bc_state, bc_taps[...], draft)
    b = bcc[:, :states].astype(bf16)
    c = bcc[:, states:].astype(bf16)
    c_ref[...] = c.astype(f32)
    zx_all = zx[...].astype(f32)
    xc = conv_rows(zx_all[:, width:], x_state[...].astype(f32), x_taps[...], draft)
    bias, rate, skip = heads3[0:1, 0:1], heads3[1:2, 0:1], heads3[2:3, 0:1]
    raw = dt[...] + bias
    step_row = jnp.maximum(raw, 0.0) + jnp.log1p(jnp.exp(-jnp.abs(raw)))
    row = lax.broadcasted_iota(jnp.int32, (tokens, tokens), 0)
    col = lax.broadcasted_iota(jnp.int32, (tokens, tokens), 1)
    same = (row // draft == col // draft) & (col <= row)
    eye = row == col
    steps_col = jnp.sum(jnp.where(eye, step_row, 0.0), axis=1, keepdims=True)
    sum_col = jnp.sum(jnp.where(same, step_row, 0.0), axis=1, keepdims=True)
    sum_row = jnp.sum(jnp.where(eye, sum_col, 0.0), axis=0, keepdims=True)
    spread = jnp.exp(jnp.where(same, (sum_row - sum_col) * rate, -1e30))
    scores = dot_nt(c, b) * spread
    xw = xc * steps_col
    y = jnp.dot(scores.astype(bf16), xw.astype(bf16), preferred_element_type=f32)

    at = lax.broadcasted_iota(jnp.int32, (tokens, 1), 0) % draft
    kept = accepted[...]
    seqs = tokens // draft
    last = jnp.where(at == kept - 1, sum_col, 0.0).reshape(seqs, draft, 1)
    last = jnp.broadcast_to(jnp.sum(last, axis=1, keepdims=True), (seqs, draft, 1))
    last = last.reshape(tokens, 1)
    coef = jnp.exp(jnp.where(at < kept, (sum_col - last) * rate, -1e30))
    keep_ref[...] = jnp.broadcast_to(jnp.exp(-last * rate), keep_ref.shape)
    xk_t = jnp.transpose(xw * coef).astype(bf16)
    lanes = 128
    in_group = lanes // draft
    group_row = lax.broadcasted_iota(jnp.int32, (lanes, states), 0) // draft
    for q in range(seqs):
        rows = slice(q * draft, (q + 1) * draft)
        g = q // in_group
        state = h0[q]
        y_ref[rows, :] = dot_nt(c_ref[rows, :].astype(bf16), state.astype(bf16))
        mine = jnp.where(
            group_row == q % in_group, b[g * lanes : (g + 1) * lanes].astype(f32), 0.0
        )
        added = jnp.dot(
            xk_t[:, g * lanes : (g + 1) * lanes],
            mine.astype(bf16),
            preferred_element_type=f32,
        )
        h_new[q] = keep_ref[q * draft : q * draft + 1, :] * state + added
    y = y + jnp.exp(-sum_col * rate) * y_ref[...] + skip * xc
    z = zx_all[:, :width]
    gated = y * (z * (1.0 / (1.0 + jnp.exp(-z))))
    u = gated * gain[...]
    u_t[...] = jnp.transpose(u).astype(bf16)
    gated_t = jnp.transpose(gated)
    ssq[...] = jnp.broadcast_to(jnp.sum(gated_t * gated_t, axis=0, keepdims=True), ssq.shape)


def mix_tokens(draft, zx, h0, *rest):
    tokens, width = zx.shape[0], zx.shape[1] // 2
    states = h0.shape[2]
    count = 2 + len(rest)
    return pl.pallas_call(
        functools.partial(mixer_kernel, draft),
        out_shape=[
            jax.ShapeDtypeStruct((width, tokens), jnp.bfloat16),
            jax.ShapeDtypeStruct((8, tokens), jnp.float32),
            jax.ShapeDtypeStruct(h0.shape, jnp.float32),
        ],
        in_specs=[pl.BlockSpec(memory_space=pltpu.VMEM)] * count,
        out_specs=[pl.BlockSpec(memory_space=pltpu.VMEM)] * 3,
        scratch_shapes=[
            pltpu.VMEM((tokens, states), jnp.float32),
            pltpu.VMEM((tokens, width), jnp.float32),
            pltpu.VMEM((tokens, states), jnp.float32),
        ],
        compiler_params=pltpu.CompilerParams(vmem_limit_bytes=VMEM_LIMIT),
        name="mixer",
    )(zx, *rest, h0)


def local(
    draft_ids, accepted, embedding, norm_gain, w_zx, w_dt, w_bc, dt_bias, decay_rate,
    skip_weight, conv_x_w, conv_x_b, conv_bc_w, conv_bc_b, gate_gain, out_w, ssm_state,
    conv_x_state, conv_bc_state,
):
    f32, bf16 = jnp.float32, jnp.bfloat16
    n = lax.axis_size("heads")
    seqs, draft = draft_ids.shape
    tokens = seqs * draft
    width = w_zx.shape[3] // 2
    own_cols = embedding.shape[1]
    model = own_cols * n
    inner = width * n
    bc_here = w_bc.shape[2]
    kernel = conv_x_w.shape[1]
    me = lax.axis_index("heads")

    rows_before = draft - (kernel - 1)
    bc_pad = jnp.pad(conv_bc_state, ((0, 0), (0, 0), (rows_before, 0), (0, 0)))
    bc_pad = bc_pad.transpose(0, 3, 1, 2).reshape(LAYERS, bc_here, tokens)
    x_pad = jnp.pad(conv_x_state, ((0, 0), (0, 0), (rows_before, 0), (0, 0)))
    x_pad = x_pad.reshape(LAYERS, tokens, width)
    bc_taps = jnp.concatenate([conv_bc_w, conv_bc_b[:, None]], axis=1).transpose(0, 2, 1)
    bc_taps = jnp.pad(bc_taps, ((0, 0), (0, 0), (0, 128 - kernel - 1)))
    x_taps = jnp.concatenate([conv_x_w, conv_x_b[:, None]], axis=1).astype(f32)
    heads3 = jnp.stack([dt_bias, decay_rate, skip_weight], axis=1)
    kept = jnp.repeat(accepted, draft)[:, None]
    w_bd = jnp.concatenate([w_bc.transpose(0, 2, 1), w_dt.transpose(0, 2, 1)], axis=1)

    parts = out_w[1].reshape(width, n, own_cols).transpose(1, 0, 2)
    part, out_whole, out_mine = lookup(
        draft_ids.reshape(1, tokens), embedding.T, out_w[0], parts, n
    )
    stream, bc_pad_all, bc_taps_all = all_gather([part, bc_pad, bc_taps], n, 1)
    stream = stream.reshape(model, tokens)
    bc_pad_all = bc_pad_all.transpose(1, 0, 2, 3).reshape(LAYERS, n * bc_here, tokens)
    bc_taps_all = bc_taps_all[..., : kernel + 1].transpose(1, 3, 0, 2)
    bc_taps_all = bc_taps_all.reshape(LAYERS, kernel + 1, n * bc_here).astype(f32)
    saved_state, saved_x, saved_bc = [], [], []
    result = None
    for layer in range(LAYERS):
        value = stream.astype(f32)
        normed = (
            value
            * rms_scale(jnp.sum(value * value, 0, keepdims=True), model)
            * norm_gain[layer][:, None]
        ).astype(bf16)
        zx = dot_tn(normed, w_zx[layer].reshape(model, -1)).astype(bf16)
        bd = jnp.dot(w_bd[layer], normed, preferred_element_type=f32).astype(bf16)
        bc_t = bd[:bc_here]
        dt = bd[bc_here:].astype(f32)
        (bc_all,) = all_gather([bc_t], n, 2 + 2 * layer)
        u_t, ssq, h_new = mix_tokens(
            draft, zx, ssm_state[layer].reshape(seqs, width, -1), dt,
            bc_all.reshape(n * bc_here, tokens), bc_pad_all[layer], bc_taps_all[layer],
            x_pad[layer], x_taps[layer], heads3[layer], kept, gate_gain[layer][None],
        )
        saved_state.append(h_new.reshape(ssm_state.shape[1:]))
        window_x = jnp.concatenate(
            [conv_x_state[layer], zx[:, width:].reshape(seqs, draft, width)], axis=1
        )
        saved_x.append(keep_rows(window_x, accepted, kernel - 1))
        window_bc = jnp.concatenate(
            [conv_bc_state[layer], bc_t.T.reshape(seqs, draft, bc_here)], axis=1
        )
        saved_bc.append(keep_rows(window_bc, accepted, kernel - 1))
        u_all, ssq_all = all_gather([u_t, ssq], n, 3 + 2 * layer)
        u_all = u_all.reshape(inner, tokens)
        scale = rms_scale(jnp.sum(ssq_all[:, 0], axis=0), inner)[None]
        if layer + 1 < LAYERS:
            mix = dot_tn(out_whole.reshape(inner, model), u_all) * scale
            stream = (value + mix).astype(bf16)
        else:
            mix = dot_tn(out_mine.reshape(inner, own_cols), u_all) * scale
            mine = lax.dynamic_slice_in_dim(stream, me * own_cols, own_cols, 0)
            result = (mine.astype(f32) + mix).astype(bf16).T
    return (result, jnp.stack(saved_state), jnp.stack(saved_x), jnp.stack(saved_bc))


def solution(mesh):
    placed = (
        P("batch", None),
        P("batch"),
        P(None, "heads"),
        P(),
        P(None, None, "heads", None),
        P(None, None, "heads"),
        P(None, None, "heads"),
        P(None, "heads"),
        P(None, "heads"),
        P(None, "heads"),
        P(None, None, "heads"),
        P(None, "heads"),
        P(None, None, "heads"),
        P(None, "heads"),
        P(None, "heads"),
        P(None, "heads", None),
        P(None, "batch", "heads", None, None),
        P(None, "batch", None, "heads"),
        P(None, "batch", None, "heads"),
    )
    return jax.shard_map(
        local,
        mesh=mesh,
        in_specs=placed,
        out_specs=(
            P("batch", "heads"),
            P(None, "batch", "heads", None, None),
            P(None, "batch", None, "heads"),
            P(None, "batch", None, "heads"),
        ),
        check_vma=False,
    )
```
